32 devices in a mesh: dp: 1 (over z), tp: 4 (over y), cp: 8 (over x, core).
Axes of the slice: x: 4, y: 4, z: 1, core: 2. Of those that a mesh axis runs over, the one named last changes fastest.
The devices are a block of a 4x4x8 slice.
Arguments:
- x: bfloat16 [8192, 3584], P(('dp', 'cp', 'tp'))
- pos: int32 [8192], P(('dp', 'cp', 'tp'))
- g1: bfloat16 [3584], replicated
- g2: bfloat16 [3584], replicated
- wq: bfloat16 [3584, 3584], P(None, 'tp')
- wk: bfloat16 [3584, 512], P(None, 'tp')
- wv: bfloat16 [3584, 512], P(None, 'tp')
- wo: bfloat16 [3584, 3584], P('tp')
- w1: bfloat16 [3584, 18944], P(None, 'tp')
- w3: bfloat16 [3584, 18944], P(None, 'tp')
- w2: bfloat16 [18944, 3584], P('tp')
Outputs:
- output: bfloat16 [8192, 3584], P(('dp', 'cp', 'tp'))
All inputs are finite; a program needn't handle non-finite values.
Results may differ from the reference program's by a relative error of at most 0.00972693.
Values are sent between devices in bfloat16 or wider.
A program may use at most 768 MiB of HBM per device.

```python
import math
import jax
import jax.numpy as jnp
from jax import lax

T = 8192
D = 3584
HQ = 28
HKV = 4
DH = 128
F = 18944
NDEV = 32
QB = 64
PIECE = T // (2 * NDEV)
GRP = HQ // HKV
EPS = 1e-5
THETA = 500000.0


def setup_inputs(seed: int = 0, part: int = 0) -> dict:
    kpart = jax.random.fold_in(jax.random.key(seed), part)
    kx, kgap, kstart = jax.random.split(kpart, 3)
    kw = jax.random.split(jax.random.key(seed + 1), 9)
    x = jax.random.normal(kx, (T, D), jnp.float32).astype(jnp.bfloat16)
    gaps = jax.random.randint(kgap, (T,), 1, 4)
    start = jax.random.randint(kstart, (), 0, T)
    seqpos = start + jnp.cumsum(gaps) - gaps[0]
    rows = jnp.arange(T)
    dev = rows // (2 * PIECE)
    off = rows % (2 * PIECE)
    piece = jnp.where(off < PIECE, dev, 2 * NDEV - 1 - dev)
    pos = seqpos[piece * PIECE + off % PIECE].astype(jnp.int32)
    qk = math.sqrt(math.sqrt(math.log(T / 16.0)))

    def nrm(k, shape, scl):
        return (jax.random.normal(k, shape, jnp.float32) * scl).astype(jnp.bfloat16)

    g1 = (1.0 + 0.3 * jax.random.normal(kw[0], (D,), jnp.float32)).astype(jnp.bfloat16)
    g2 = (1.0 + 0.3 * jax.random.normal(kw[1], (D,), jnp.float32)).astype(jnp.bfloat16)
    wq = nrm(kw[2], (D, HQ * DH), qk / math.sqrt(D))
    wk = nrm(kw[3], (D, HKV * DH), qk / math.sqrt(D))
    wv = nrm(kw[4], (D, HKV * DH), 1.0 / math.sqrt(D))
    wo = nrm(kw[5], (HQ * DH, D), 2.0 / math.sqrt(HQ * DH))
    w1 = nrm(kw[6], (D, F), 1.0 / math.sqrt(D))
    w3 = nrm(kw[7], (D, F), 1.0 / math.sqrt(D))
    w2 = nrm(kw[8], (F, D), 1.0 / math.sqrt(F))
    return dict(x=x, pos=pos, g1=g1, g2=g2, wq=wq, wk=wk, wv=wv, wo=wo, w1=w1, w3=w3, w2=w2)


def rms_norm(v, g):
    vf = v.astype(jnp.float32)
    inv = lax.rsqrt(jnp.mean(vf * vf, axis=-1, keepdims=True) + EPS)
    return (vf * inv * g.astype(jnp.float32)).astype(jnp.bfloat16)


def rope(y, p):
    half = DH // 2
    freq = 1.0 / (THETA ** (jnp.arange(0, DH, 2, dtype=jnp.float32) / DH))
    ang = p.astype(jnp.float32)[..., None] * freq
    c = jnp.cos(ang)[..., None, :]
    s = jnp.sin(ang)[..., None, :]
    y1 = y[..., :half]
    y2 = y[..., half:]
    return jnp.concatenate([y1 * c - y2 * s, y2 * c + y1 * s], axis=-1)


def attention(q, k, v, p):
    qr = q.reshape(T // QB, QB, HKV, GRP, DH)
    pr = p.reshape(T // QB, QB)
    kf = k.astype(jnp.float32)
    vf = v.astype(jnp.float32)
    scale = 1.0 / math.sqrt(DH)

    def blk(qp):
        qq, pp = qp
        s = jnp.einsum('qkgd,skd->kgqs', qq.astype(jnp.float32), kf) * scale
        s = jnp.where(p[None, None, None, :] <= pp[None, None, :, None], s, -1e30)
        e = jnp.exp(s - jnp.max(s, axis=-1, keepdims=True))
        w = (e / jnp.sum(e, axis=-1, keepdims=True)).astype(jnp.bfloat16)
        o = jnp.einsum('kgqs,skd->qkgd', w.astype(jnp.float32), vf)
        return o.astype(jnp.bfloat16)

    return lax.map(blk, (qr, pr)).reshape(T, HQ * DH)


def reference(x, pos, g1, g2, wq, wk, wv, wo, w1, w3, w2):
    a = rms_norm(x, g1)
    q = rope(jnp.dot(a, wq, preferred_element_type=jnp.float32).reshape(T, HQ, DH), pos).astype(jnp.bfloat16)
    k = rope(jnp.dot(a, wk, preferred_element_type=jnp.float32).reshape(T, HKV, DH), pos).astype(jnp.bfloat16)
    v = jnp.dot(a, wv, preferred_element_type=jnp.float32).astype(jnp.bfloat16).reshape(T, HKV, DH)
    o = attention(q, k, v, pos)
    h1 = (x.astype(jnp.float32) + jnp.dot(o, wo, preferred_element_type=jnp.float32)).astype(jnp.bfloat16)
    b = rms_norm(h1, g2)
    hid = (jax.nn.silu(jnp.dot(b, w1, preferred_element_type=jnp.float32)) * jnp.dot(b, w3, preferred_element_type=jnp.float32)).astype(jnp.bfloat16)
    return (h1.astype(jnp.float32) + jnp.dot(hid, w2, preferred_element_type=jnp.float32)).astype(jnp.bfloat16)
```

```python
import functools
import math
import jax
import jax.numpy as jnp
from jax import lax
from jax.experimental import pallas as pl
from jax.experimental.pallas import tpu as pltpu
from jax.sharding import PartitionSpec as P

DH = 128
EPS = 1e-5
THETA = 500000.0
NEG = -1e30


def rms_norm(v, g):
    vf = v.astype(jnp.float32)
    inv = lax.rsqrt(jnp.mean(vf * vf, axis=-1, keepdims=True) + EPS)
    return (vf * inv * g.astype(jnp.float32)).astype(jnp.bfloat16)


def rope(y, p):
    half = DH // 2
    freq = 1.0 / (THETA ** (jnp.arange(0, DH, 2, dtype=jnp.float32) / DH))
    ang = p.astype(jnp.float32)[..., None] * freq
    c = jnp.cos(ang)[..., None, :]
    s = jnp.sin(ang)[..., None, :]
    y1 = y[..., :half]
    y2 = y[..., half:]
    return jnp.concatenate([y1 * c - y2 * s, y2 * c + y1 * s], axis=-1)


def attn_body(rev, npiece, nblk, c_ref, q_ref, *refs):
    if rev:
        kva_ref, kvb_ref, o_ref, acc, m_s, l_s = refs
    else:
        kva_ref, o_ref, acc, m_s, l_s = refs
    c = c_ref[0]
    n = q_ref.shape[0]
    bk = n
    coef = math.log2(math.e) / math.sqrt(DH)
    q = q_ref[...]

    def step(kv_ref, i, diag, first):
        k = kv_ref[pl.ds(i * bk, bk), :DH]
        v = kv_ref[pl.ds(i * bk, bk), DH:]
        s = lax.dot_general(q, k, (((1,), (1,)), ((), ())), preferred_element_type=jnp.float32)
        if diag:
            r = lax.broadcasted_iota(jnp.int32, (n, bk), 0)
            t = lax.broadcasted_iota(jnp.int32, (n, bk), 1)
            if rev:
                piece = n // npiece
                r = (npiece - 1 - r // piece) * piece + r % piece
                t = (npiece - 1 - t // piece) * piece + t % piece
            s = jnp.where(t <= r, s, NEG)
        mx = jnp.max(s, axis=1, keepdims=True)
        if first:
            m = mx
        else:
            m0 = m_s[:, :1]
            m = jnp.maximum(m0, mx)
        p = jnp.exp2((s - m) * coef)
        part = p[:, :128]
        for u in range(1, bk // 128):
            part = part + p[:, u * 128:(u + 1) * 128]
        pv = jnp.dot(p.astype(jnp.bfloat16), v, preferred_element_type=jnp.float32)
        if first:
            l_s[...] = part
            acc[...] = pv
        else:
            al = jnp.exp2((m0 - m) * coef)
            l_s[...] = l_s[...] * al + part
            acc[...] = acc[...] * al + pv
        m_s[...] = jnp.broadcast_to(m, m_s.shape)

    step(kvb_ref if rev else kva_ref, c, True, True)
    if rev:
        @pl.loop(0, nblk)
        def _(i):
            step(kva_ref, i, False, False)

        @pl.loop(c + 1, nblk)
        def _(i):
            step(kvb_ref, i, False, False)
    else:
        @pl.loop(0, c)
        def _(i):
            step(kva_ref, i, False, False)
    l = jnp.sum(l_s[...], axis=1, keepdims=True)
    o_ref[...] = (acc[...] / l).astype(o_ref.dtype)


def attend(rev, npiece, nblk, c, q, *kvs):
    n, w = q.shape
    heads = w // DH
    units = (nblk + 1 + nblk // 2) if rev else nblk // 2 + 1
    gs = pltpu.PrefetchScalarGridSpec(
        num_scalar_prefetch=1,
        grid=(heads,),
        in_specs=[pl.BlockSpec((n, DH), lambda h, c: (0, h))]
        + [pl.BlockSpec(kv.shape, lambda h, c: (0, 0)) for kv in kvs],
        out_specs=pl.BlockSpec((n, DH), lambda h, c: (0, h)),
        scratch_shapes=[pltpu.VMEM((n, DH), jnp.float32)] * 3,
    )
    return pl.pallas_call(
        functools.partial(attn_body, rev, npiece, nblk),
        grid_spec=gs,
        out_shape=jax.ShapeDtypeStruct((n, w), jnp.bfloat16),
        compiler_params=pltpu.CompilerParams(dimension_semantics=("arbitrary",)),
        cost_estimate=pl.CostEstimate(
            flops=units * heads * n * n * DH * 4 * 3, bytes_accessed=3 * n * w * 2 + sum(kv.size * 2 for kv in kvs),
            transcendentals=units * heads * n * n),
        name="attn_b" if rev else "attn_a",
    )(c, q, *kvs)


def solution(mesh):
    tok = P(('dp', 'cp', 'tp'), None)
    col = P(None, 'tp')
    row = P('tp', None)
    ntp = mesh.shape['tp']
    ncp = mesh.shape['cp']

    def local(x, pos, g1, g2, wq, wk, wv, wo, w1, w3, w2):
        f32 = jnp.float32
        half = x.shape[0] // 2
        xs = [x[:half], x[half:]]
        pg = lax.all_gather(pos, 'tp', axis=0).reshape(ntp, 2, half)
        cidx = lax.axis_index('cp').astype(jnp.int32).reshape(1)
        ag = lambda u: lax.all_gather(u, 'tp', axis=0, tiled=True)
        dot = lambda u, w: jnp.dot(u, w, preferred_element_type=f32)

        an0 = rms_norm(xs[0], g1)
        an0, xb = lax.optimization_barrier((an0, xs[1]))
        ans = [an0, rms_norm(xb, g1)]
        qs, kvs = [], []
        for i in range(2):
            a = ag(ans[i])
            p = pg[:, i].reshape(-1)
            nr = a.shape[0]
            k = rope(dot(a, wk).reshape(nr, -1, DH), p).astype(jnp.bfloat16).reshape(nr, -1)
            v = dot(a, wv).astype(jnp.bfloat16)
            kvs.append(lax.all_gather(jnp.concatenate([k, v], axis=1), 'cp', axis=0, tiled=True))
            qs.append(rope(dot(a, wq).reshape(nr, -1, DH), p).astype(jnp.bfloat16).reshape(nr, -1))

        outs = []
        oa = attend(False, ntp, ncp, cidx, qs[0], kvs[0])
        oa, qb = lax.optimization_barrier((oa, qs[1]))
        ya = dot(oa, wo).astype(jnp.bfloat16)
        ya, qb = lax.optimization_barrier((ya, qb))
        os = [oa, attend(True, ntp, ncp, cidx, qb, kvs[0], kvs[1])]
        bn = None
        for i in range(2):
            y = ya if i == 0 else dot(os[i], wo).astype(jnp.bfloat16)
            y = lax.psum_scatter(y, 'tp', scatter_dimension=0, tiled=True)
            if bn is not None:
                y, bn = lax.optimization_barrier((y, bn))
            h1 = (xs[i].astype(f32) + y.astype(f32)).astype(jnp.bfloat16)
            bn = rms_norm(h1, g2)
            b = ag(bn)
            hid = (jax.nn.silu(dot(b, w1)) * dot(b, w3)).astype(jnp.bfloat16)
            z = lax.psum_scatter(dot(hid, w2).astype(jnp.bfloat16), 'tp', scatter_dimension=0, tiled=True)
            outs.append((h1.astype(f32) + z.astype(f32)).astype(jnp.bfloat16))
        return jnp.concatenate(outs, axis=0)

    return jax.shard_map(local, mesh=mesh, in_specs=(tok, P(('dp', 'cp', 'tp')), P(None), P(None), col, col, col, row, col, col, row), out_specs=tok, check_vma=False)
```

```python
import functools
import math
import jax
import jax.numpy as jnp
from jax import lax
from jax.experimental import pallas as pl
from jax.experimental.pallas import tpu as pltpu
from jax.sharding import PartitionSpec as P

DH = 128
EPS = 1e-5
THETA = 500000.0
NEG = -1e30
PAIR = 2


def rms_norm(v, g):
    vf = v.astype(jnp.float32)
    inv = lax.rsqrt(jnp.mean(vf * vf, axis=-1, keepdims=True) + EPS)
    return (vf * inv * g.astype(jnp.float32)).astype(jnp.bfloat16)


def rope_tables(p):
    freq = 1.0 / (THETA ** (jnp.arange(0, DH, 2, dtype=jnp.float32) / DH))
    ang = p.astype(jnp.float32)[:, None] * freq
    c, s = jnp.cos(ang), jnp.sin(ang)
    return jnp.concatenate([c, c], axis=1), jnp.concatenate([-s, s], axis=1)


def proj_body(roped, a_ref, w_ref, c_ref, s_ref, o_ref):
    nb, piece, d = a_ref.shape
    y = jnp.dot(a_ref[...].reshape(nb * piece, d), w_ref[...], preferred_element_type=jnp.float32)
    for t in range(y.shape[1] // DH):
        yt = y[:, t * DH:(t + 1) * DH]
        if t < roped:
            yt = yt * c_ref[...] + pltpu.roll(yt, DH // 2, 1) * s_ref[...]
        o_ref[:, t * DH:(t + 1) * DH] = yt.astype(o_ref.dtype)


def proj(a, i, w, c, s, roped, tn):
    nb, _, piece, d = a.shape
    n = nb * piece
    wd = w.shape[1]
    return pl.pallas_call(
        functools.partial(proj_body, roped),
        grid=(pl.cdiv(wd, tn),),
        in_specs=[
            pl.BlockSpec((nb, None, piece, d), lambda t: (0, i, 0, 0)),
            pl.BlockSpec((d, tn), lambda t: (0, t)),
            pl.BlockSpec((n, DH), lambda t: (0, 0)),
            pl.BlockSpec((n, DH), lambda t: (0, 0)),
        ],
        out_specs=pl.BlockSpec((n, tn), lambda t: (0, t)),
        out_shape=jax.ShapeDtypeStruct((n, wd), jnp.bfloat16),
        compiler_params=pltpu.CompilerParams(dimension_semantics=("arbitrary",)),
        cost_estimate=pl.CostEstimate(flops=2 * n * d * wd, bytes_accessed=2 * (n * d + d * wd + n * wd), transcendentals=0),
    )(a, w, c, s)


def mm_body(x_ref, w_ref, o_ref):
    o_ref[...] = jnp.dot(x_ref[...], w_ref[...], preferred_element_type=jnp.float32).astype(o_ref.dtype)


def mm(x, w, tn):
    n, d = x.shape
    wd = w.shape[1]
    return pl.pallas_call(
        mm_body,
        grid=(pl.cdiv(wd, tn),),
        in_specs=[pl.BlockSpec((n, d), lambda t: (0, 0)), pl.BlockSpec((d, tn), lambda t: (0, t))],
        out_specs=pl.BlockSpec((n, tn), lambda t: (0, t)),
        out_shape=jax.ShapeDtypeStruct((n, wd), jnp.bfloat16),
        compiler_params=pltpu.CompilerParams(dimension_semantics=("arbitrary",)),
        cost_estimate=pl.CostEstimate(flops=2 * n * d * wd, bytes_accessed=2 * (n * d + d * wd + n * wd), transcendentals=0),
    )(x, w)


def gate_body(b_ref, w1_ref, w3_ref, o_ref):
    n = b_ref.shape[0]
    step = n // 2
    for r in range(0, n, step):
        b = b_ref[r:r + step, :]
        g = jnp.dot(b, w1_ref[...], preferred_element_type=jnp.float32)
        u = jnp.dot(b, w3_ref[...], preferred_element_type=jnp.float32)
        o_ref[r:r + step, :] = (jax.nn.silu(g) * u).astype(o_ref.dtype)


def gate_up(b, w1, w3, tn):
    n, d = b.shape
    wd = w1.shape[1]
    return pl.pallas_call(
        gate_body,
        grid=(pl.cdiv(wd, tn),),
        in_specs=[pl.BlockSpec((n, d), lambda t: (0, 0)), pl.BlockSpec((d, tn), lambda t: (0, t)), pl.BlockSpec((d, tn), lambda t: (0, t))],
        out_specs=pl.BlockSpec((n, tn), lambda t: (0, t)),
        out_shape=jax.ShapeDtypeStruct((n, wd), jnp.bfloat16),
        compiler_params=pltpu.CompilerParams(dimension_semantics=("arbitrary",)),
        cost_estimate=pl.CostEstimate(flops=4 * n * d * wd, bytes_accessed=2 * (n * d + 2 * d * wd + n * wd), transcendentals=n * wd),
        name="gate_up",
    )(b, w1, w3)


def attn_body(rev, npiece, nblk, c_ref, q_ref, *refs):
    if rev:
        kva_ref, kvb_ref, o_ref, kv_s, kt_s, q_s, acc, m_s, l_s, sem = refs
    else:
        kva_ref, o_ref, kv_s, kt_s, q_s, acc, m_s, l_s, sem = refs
    c = c_ref[0]
    g = pl.program_id(0)
    piece, w = q_ref.shape
    heads = w // DH
    n = piece * npiece
    rows_all = heads * piece
    na = nblk * n
    coef = math.log2(math.e) / math.sqrt(DH)
    nt = n // DH

    @pl.when(g == 0)
    def _():
        cps = [pltpu.make_async_copy(kva_ref, kv_s.at[pl.ds(0, na)], sem.at[0])]
        if rev:
            cps.append(pltpu.make_async_copy(kvb_ref, kv_s.at[pl.ds(na, na)], sem.at[1]))
        for cp in cps:
            cp.start()
        for cp in cps:
            cp.wait()

        @pl.loop(0, kt_s.shape[0])
        def _(i):
            k = kv_s[pl.ds(pl.multiple_of(i * n, n), n), :DH]
            kt_s[i] = k.T

    for h in range(heads):
        q_s[h * piece:(h + 1) * piece, :] = q_ref[:, h * DH:(h + 1) * DH]

    def step(blocks, diag, first):
        kvs = [(kt_s[i], kv_s[pl.ds(pl.multiple_of(i * n, n), n), DH:]) for i in blocks]
        for r0 in (0,):
            rows = pl.ds(r0, rows_all)
            q = q_s[rows, :]
            tiles = []
            for k, _ in kvs:
                s = jnp.dot(q, k, preferred_element_type=jnp.float32)
                if diag:
                    r = lax.broadcasted_iota(jnp.int32, s.shape, 0) % piece
                    t = lax.broadcasted_iota(jnp.int32, s.shape, 1)
                    u = t // piece
                    ahead = (u < g) if rev else (u > g)
                    keep = jnp.logical_and(jnp.logical_not(ahead), jnp.logical_or(u != g, t % piece <= r))
                    s = jnp.where(keep, s, NEG)
                tiles.append([s[:, u * DH:(u + 1) * DH] for u in range(nt)])
            flat = [t for ts in tiles for t in ts]
            mx = functools.reduce(jnp.maximum, flat)
            mx = jnp.max(mx, axis=1, keepdims=True)
            if first:
                m = jnp.broadcast_to(mx, (rows_all, DH))
            else:
                m0 = m_s[rows, :]
                m = jnp.maximum(m0, mx)
            part = None
            pv = None
            for ts, (_, v) in zip(tiles, kvs):
                ps = [jnp.exp2((t - m) * coef) for t in ts]
                for p in ps:
                    part = p if part is None else part + p
                pb = jnp.concatenate([p.astype(jnp.bfloat16) for p in ps], axis=1)
                d = jnp.dot(pb, v, preferred_element_type=jnp.float32)
                pv = d if pv is None else pv + d
            if first:
                l_s[rows, :] = part
                acc[rows, :] = pv
            else:
                al = jnp.exp2((m0 - m) * coef)
                l_s[rows, :] = l_s[rows, :] * al + part
                acc[rows, :] = acc[rows, :] * al + pv
            m_s[rows, :] = m

    step([c + nblk if rev else c], True, True)
    count = (2 * nblk - 1 - c) if rev else c
    idx = (lambda t: jnp.where(t < nblk, t, t + c + 1)) if rev else (lambda t: t)

    @pl.loop(0, count // PAIR)
    def _(t):
        step([idx(PAIR * t + u) for u in range(PAIR)], False, False)

    if PAIR > 1:
        @pl.loop(count // PAIR * PAIR, count)
        def _(t):
            step([idx(t)], False, False)
    for h in range(heads):
        rows = slice(h * piece, (h + 1) * piece)
        l = jnp.sum(l_s[rows, :], axis=1, keepdims=True)
        o_ref[:, h * DH:(h + 1) * DH] = (acc[rows, :] / l).astype(o_ref.dtype)


def attend(rev, npiece, nblk, c, q, *kvs):
    n, w = q.shape[0] // 2, q.shape[1]
    piece = n // npiece
    off = npiece if rev else 0
    heads = w // DH
    units = (nblk + 1 + nblk // 2) if rev else nblk // 2 + 1
    blocks = len(kvs) * nblk
    gs = pltpu.PrefetchScalarGridSpec(
        num_scalar_prefetch=1,
        grid=(npiece,),
        in_specs=[pl.BlockSpec((piece, w), lambda g, c: (g + off, 0))]
        + [pl.BlockSpec(memory_space=pl.ANY) for kv in kvs],
        out_specs=pl.BlockSpec((piece, w), lambda g, c: (g, 0)),
        scratch_shapes=[
            pltpu.VMEM((blocks * n, 2 * DH), jnp.bfloat16),
            pltpu.VMEM((blocks, DH, n), jnp.bfloat16),
            pltpu.VMEM((heads * piece, DH), jnp.bfloat16),
        ] + [pltpu.VMEM((heads * piece, DH), jnp.float32)] * 3 + [pltpu.SemaphoreType.DMA((2,))],
    )
    return pl.pallas_call(
        functools.partial(attn_body, rev, npiece, nblk),
        grid_spec=gs,
        out_shape=jax.ShapeDtypeStruct((n, w), jnp.bfloat16),
        compiler_params=pltpu.CompilerParams(dimension_semantics=("arbitrary",)),
        cost_estimate=pl.CostEstimate(
            flops=units * heads * n * n * DH * 4 * 3, bytes_accessed=3 * n * w * 2 + sum(kv.size * 2 for kv in kvs),
            transcendentals=units * heads * n * n),
        name="attn_b" if rev else "attn_a",
    )(c, q, *kvs)


def solution(mesh):
    tok = P(('dp', 'cp', 'tp'), None)
    col = P(None, 'tp')
    row = P('tp', None)
    ntp = mesh.shape['tp']
    ncp = mesh.shape['cp']

    def local(x, pos, g1, g2, wq, wk, wv, wo, w1, w3, w2):
        f32 = jnp.float32
        half = x.shape[0] // 2
        xs = [x[:half], x[half:]]
        bar = lax.optimization_barrier
        cidx = lax.axis_index('cp').astype(jnp.int32).reshape(1)
        ag = lambda u: lax.all_gather(u, 'tp', axis=0, tiled=True)
        rs = lambda u: lax.psum_scatter(u, 'tp', scatter_dimension=0, tiled=True)

        a = ag(rms_norm(x, g1)).reshape(ntp, 2, half, -1)
        pg = lax.all_gather(pos, 'tp', axis=0).reshape(ntp, 2, half)
        wkv = jnp.concatenate([wk, wv], axis=1)
        tabs = [rope_tables(pg[:, i].reshape(-1)) for i in range(2)]
        kvs = [proj(a, i, wkv, *tabs[i], 1, 2 * DH) for i in range(2)]
        kvg = [lax.all_gather(kv, 'cp', axis=0, tiled=True) for kv in kvs]
        qs = jnp.concatenate([proj(a, i, wq, *tabs[i], 2, 2 * DH) for i in range(2)], axis=0)

        oa = attend(False, ntp, ncp, cidx, qs, kvg[0])
        ya = mm(oa, wo, 512)
        ya, qs = bar((ya, qs))
        yb = mm(attend(True, ntp, ncp, cidx, qs, *kvg), wo, 512)
        h0 = (xs[0].astype(f32) + rs(ya).astype(f32)).astype(jnp.bfloat16)
        b0 = rms_norm(h0, g2)
        yb, b0 = bar((yb, b0))
        b0 = ag(b0)
        yb = rs(yb)
        m0, yb = bar((gate_up(b0, w1, w3, 2 * DH), yb))
        h1 = (xs[1].astype(f32) + yb.astype(f32)).astype(jnp.bfloat16)
        b1 = rms_norm(h1, g2)
        m0, b1 = bar((m0, b1))
        z0 = mm(m0, w2, 2 * DH)
        z1 = mm(gate_up(ag(b1), w1, w3, 2 * DH), w2, 2 * DH)
        outs = []
        for h, z in ((h0, z0), (h1, z1)):
            z = rs(z)
            outs.append((h.astype(f32) + z.astype(f32)).astype(jnp.bfloat16))
        return jnp.concatenate(outs, axis=0)

    return jax.shard_map(local, mesh=mesh, in_specs=(tok, P(('dp', 'cp', 'tp')), P(None), P(None), col, col, col, row, col, col, row), out_specs=tok, check_vma=False)
```

```python
import functools
import math
import jax
import jax.numpy as jnp
from jax import lax
from jax.experimental import pallas as pl
from jax.experimental.pallas import tpu as pltpu
from jax.sharding import PartitionSpec as P

DH = 128
EPS = 1e-5
THETA = 500000.0
NEG = -1e30
PAIR = 2


def rms_norm(v, g):
    vf = v.astype(jnp.float32)
    inv = lax.rsqrt(jnp.mean(vf * vf, axis=-1, keepdims=True) + EPS)
    return (vf * inv * g.astype(jnp.float32)).astype(jnp.bfloat16)


def rope_tables(p):
    freq = 1.0 / (THETA ** (jnp.arange(0, DH, 2, dtype=jnp.float32) / DH))
    ang = p.astype(jnp.float32)[:, None] * freq
    c, s = jnp.cos(ang), jnp.sin(ang)
    return jnp.concatenate([c, c], axis=1), jnp.concatenate([-s, s], axis=1)


def proj_body(roped, a_ref, w_ref, c_ref, s_ref, o_ref):
    nb, piece, d = a_ref.shape
    y = jnp.dot(a_ref[...].reshape(nb * piece, d), w_ref[...], preferred_element_type=jnp.float32)
    for t in range(y.shape[1] // DH):
        yt = y[:, t * DH:(t + 1) * DH]
        if t < roped:
            yt = yt * c_ref[...] + pltpu.roll(yt, DH // 2, 1) * s_ref[...]
        o_ref[:, t * DH:(t + 1) * DH] = yt.astype(o_ref.dtype)


def proj(a, i, w, c, s, roped, tn):
    nb, _, piece, d = a.shape
    n = nb * piece
    wd = w.shape[1]
    return pl.pallas_call(
        functools.partial(proj_body, roped),
        grid=(pl.cdiv(wd, tn),),
        in_specs=[
            pl.BlockSpec((nb, None, piece, d), lambda t: (0, i, 0, 0)),
            pl.BlockSpec((d, tn), lambda t: (0, t)),
            pl.BlockSpec((n, DH), lambda t: (0, 0)),
            pl.BlockSpec((n, DH), lambda t: (0, 0)),
        ],
        out_specs=pl.BlockSpec((n, tn), lambda t: (0, t)),
        out_shape=jax.ShapeDtypeStruct((n, wd), jnp.bfloat16),
        compiler_params=pltpu.CompilerParams(dimension_semantics=("arbitrary",)),
        cost_estimate=pl.CostEstimate(flops=2 * n * d * wd, bytes_accessed=2 * (n * d + d * wd + n * wd), transcendentals=0),
    )(a, w, c, s)


def mm_body(x_ref, w_ref, o_ref):
    o_ref[...] = jnp.dot(x_ref[...], w_ref[...], preferred_element_type=jnp.float32).astype(o_ref.dtype)


def mm(x, w, tn):
    n, d = x.shape
    wd = w.shape[1]
    return pl.pallas_call(
        mm_body,
        grid=(pl.cdiv(wd, tn),),
        in_specs=[pl.BlockSpec((n, d), lambda t: (0, 0)), pl.BlockSpec((d, tn), lambda t: (0, t))],
        out_specs=pl.BlockSpec((n, tn), lambda t: (0, t)),
        out_shape=jax.ShapeDtypeStruct((n, wd), jnp.bfloat16),
        compiler_params=pltpu.CompilerParams(dimension_semantics=("arbitrary",)),
        cost_estimate=pl.CostEstimate(flops=2 * n * d * wd, bytes_accessed=2 * (n * d + d * wd + n * wd), transcendentals=0),
    )(x, w)


def down_scatter_body(ntp, m_ref, w_ref, h_ref, o_ref, z_s, far_in, fwd, near_in, far_send, far_recv, fwd_send, fwd_recv):
    t = pl.program_id(0)
    last = pl.num_programs(0) - 1
    me = lax.axis_index("tp")
    side = (lax.rem(me + 1, ntp), lax.rem(me + ntp - 1, ntp))
    far = lax.rem(me + 2, ntp)
    tn = w_ref.shape[1]
    piece = h_ref.shape[0]
    half = piece // 2

    def cols(u):
        return pl.ds(pl.multiple_of(u * tn, tn), tn)

    def rows(owner, off, size):
        return pl.ds(pl.multiple_of(owner * piece + off, half), size)

    def far_copy(d, u):
        return pltpu.make_async_remote_copy(
            src_ref=z_s.at[rows(far, d * half, half), cols(u)], dst_ref=far_in.at[d, :, cols(u)],
            send_sem=far_send.at[d], recv_sem=far_recv.at[d, u],
            device_id={"tp": side[d]}, device_id_type=pl.DeviceIdType.MESH)

    def fwd_copy(d, u):
        return pltpu.make_async_remote_copy(
            src_ref=fwd.at[d, :, cols(u)], dst_ref=near_in.at[d, :, cols(u)],
            send_sem=fwd_send.at[d], recv_sem=fwd_recv.at[d],
            device_id={"tp": side[d]}, device_id_type=pl.DeviceIdType.MESH)

    def send_far(u):
        for d in range(2):
            far_copy(d, u).start()

    def send_fwd(u):
        for d in range(2):
            fwd_copy(d, u).start()

    def add(u):
        for d in range(2):
            far_copy(d, u).wait_recv()
            mine = slice(d * half, (d + 1) * half)
            rest = slice((1 - d) * half, (2 - d) * half)
            got = far_in[d, :, cols(u)].astype(jnp.float32)
            own = z_s[rows(side[d], d * half, half), cols(u)].astype(jnp.float32)
            fwd[d, mine, cols(u)] = (own + got).astype(fwd.dtype)
            fwd[d, rest, cols(u)] = z_s[rows(side[d], (1 - d) * half, half), cols(u)]

    @pl.when(t == 0)
    def _():
        bar = pltpu.get_barrier_semaphore()
        for d in range(2):
            pl.semaphore_signal(bar, inc=1, device_id={"tp": side[d]}, device_id_type=pl.DeviceIdType.MESH)
        pl.semaphore_wait(bar, 2)

    z_s[:, cols(t)] = jnp.dot(m_ref[...], w_ref[...], preferred_element_type=jnp.float32).astype(z_s.dtype)

    @pl.when(t >= 1)
    def _():
        send_far(t - 1)

    @pl.when(t >= 3)
    def _():
        add(t - 3)

    @pl.when(t >= 4)
    def _():
        send_fwd(t - 4)

    @pl.when(t == last)
    def _():
        send_far(last)
        send_fwd(last - 3)

        @pl.loop(last - 2, last + 1)
        def _(u):
            add(u)
            send_fwd(u)

        for d in range(2):
            whole = pltpu.make_async_remote_copy(
                src_ref=fwd.at[d], dst_ref=near_in.at[d], send_sem=fwd_send.at[d], recv_sem=fwd_recv.at[d],
                device_id={"tp": side[d]}, device_id_type=pl.DeviceIdType.MESH)
            whole.wait()
            pltpu.make_async_remote_copy(
                src_ref=far_in.at[d], dst_ref=far_in.at[d], send_sem=far_send.at[d], recv_sem=far_recv.at[d, 0],
                device_id={"tp": side[d]}, device_id_type=pl.DeviceIdType.MESH).wait_send()

        @pl.loop(0, last + 1)
        def _(u):
            own = z_s[rows(me, 0, piece), cols(u)].astype(jnp.float32)
            z = own + near_in[0, :, cols(u)].astype(jnp.float32) + near_in[1, :, cols(u)].astype(jnp.float32)
            o_ref[:, cols(u)] = (h_ref[:, cols(u)].astype(jnp.float32) + z).astype(o_ref.dtype)


def down_scatter(ntp, m, w, h, tn):
    n, d = m.shape
    wd = w.shape[1]
    piece = n // ntp
    tiles = wd // tn
    bf = jnp.bfloat16
    return pl.pallas_call(
        functools.partial(down_scatter_body, ntp),
        grid=(tiles,),
        in_specs=[pl.BlockSpec((n, d), lambda t: (0, 0)), pl.BlockSpec((d, tn), lambda t: (0, t)), pl.BlockSpec((piece, wd), lambda t: (0, 0))],
        out_specs=pl.BlockSpec((piece, wd), lambda t: (0, 0)),
        out_shape=jax.ShapeDtypeStruct((piece, wd), bf),
        scratch_shapes=[
            pltpu.VMEM((n, wd), bf), pltpu.VMEM((2, piece // 2, wd), bf), pltpu.VMEM((2, piece, wd), bf), pltpu.VMEM((2, piece, wd), bf),
            pltpu.SemaphoreType.DMA((2,)), pltpu.SemaphoreType.DMA((2, tiles)), pltpu.SemaphoreType.DMA((2,)), pltpu.SemaphoreType.DMA((2,)),
        ],
        compiler_params=pltpu.CompilerParams(dimension_semantics=("arbitrary",), collective_id=0, has_side_effects=True),
        cost_estimate=pl.CostEstimate(flops=2 * n * d * wd, bytes_accessed=2 * (n * d + d * wd + n * wd), transcendentals=0),
        name="down_scatter",
    )(m, w, h)


def gate_body(b_ref, w1_ref, w3_ref, o_ref):
    n = b_ref.shape[0]
    step = n // 2
    for r in range(0, n, step):
        b = b_ref[r:r + step, :]
        g = jnp.dot(b, w1_ref[...], preferred_element_type=jnp.float32)
        u = jnp.dot(b, w3_ref[...], preferred_element_type=jnp.float32)
        o_ref[r:r + step, :] = (jax.nn.silu(g) * u).astype(o_ref.dtype)


def gate_up(b, w1, w3, tn):
    n, d = b.shape
    wd = w1.shape[1]
    return pl.pallas_call(
        gate_body,
        grid=(pl.cdiv(wd, tn),),
        in_specs=[pl.BlockSpec((n, d), lambda t: (0, 0)), pl.BlockSpec((d, tn), lambda t: (0, t)), pl.BlockSpec((d, tn), lambda t: (0, t))],
        out_specs=pl.BlockSpec((n, tn), lambda t: (0, t)),
        out_shape=jax.ShapeDtypeStruct((n, wd), jnp.bfloat16),
        compiler_params=pltpu.CompilerParams(dimension_semantics=("arbitrary",)),
        cost_estimate=pl.CostEstimate(flops=4 * n * d * wd, bytes_accessed=2 * (n * d + 2 * d * wd + n * wd), transcendentals=n * wd),
        name="gate_up",
    )(b, w1, w3)


def attn_body(rev, npiece, nblk, c_ref, q_ref, *refs):
    if rev:
        kva_ref, kvb_ref, o_ref, kv_s, kt_s, q_s, acc, m_s, l_s, sem = refs
    else:
        kva_ref, o_ref, kv_s, kt_s, q_s, acc, m_s, l_s, sem = refs
    c = c_ref[0]
    g = pl.program_id(0)
    piece, w = q_ref.shape
    heads = w // DH
    n = piece * npiece
    rows_all = heads * piece
    na = nblk * n
    coef = math.log2(math.e) / math.sqrt(DH)
    nt = n // DH

    @pl.when(g == 0)
    def _():
        cps = [pltpu.make_async_copy(kva_ref, kv_s.at[pl.ds(0, na)], sem.at[0])]
        if rev:
            cps.append(pltpu.make_async_copy(kvb_ref, kv_s.at[pl.ds(na, na)], sem.at[1]))
        for cp in cps:
            cp.start()
        for cp in cps:
            cp.wait()

        @pl.loop(0, kt_s.shape[0])
        def _(i):
            k = kv_s[pl.ds(pl.multiple_of(i * n, n), n), :DH]
            kt_s[i] = k.T

    for h in range(heads):
        q_s[h * piece:(h + 1) * piece, :] = q_ref[:, h * DH:(h + 1) * DH]

    def step(blocks, diag, first):
        kvs = [(kt_s[i], kv_s[pl.ds(pl.multiple_of(i * n, n), n), DH:]) for i in blocks]
        for r0 in (0,):
            rows = pl.ds(r0, rows_all)
            q = q_s[rows, :]
            tiles = []
            for k, _ in kvs:
                s = jnp.dot(q, k, preferred_element_type=jnp.float32)
                if diag:
                    r = lax.broadcasted_iota(jnp.int32, s.shape, 0) % piece
                    t = lax.broadcasted_iota(jnp.int32, s.shape, 1)
                    u = t // piece
                    ahead = (u < g) if rev else (u > g)
                    keep = jnp.logical_and(jnp.logical_not(ahead), jnp.logical_or(u != g, t % piece <= r))
                    s = jnp.where(keep, s, NEG)
                tiles.append([s[:, u * DH:(u + 1) * DH] for u in range(nt)])
            flat = [t for ts in tiles for t in ts]
            mx = functools.reduce(jnp.maximum, flat)
            mx = jnp.max(mx, axis=1, keepdims=True)
            if first:
                m = jnp.broadcast_to(mx, (rows_all, DH))
            else:
                m0 = m_s[rows, :]
                m = jnp.maximum(m0, mx)
            part = None
            pv = None
            for ts, (_, v) in zip(tiles, kvs):
                ps = [jnp.exp2((t - m) * coef) for t in ts]
                for p in ps:
                    part = p if part is None else part + p
                pb = jnp.concatenate([p.astype(jnp.bfloat16) for p in ps], axis=1)
                d = jnp.dot(pb, v, preferred_element_type=jnp.float32)
                pv = d if pv is None else pv + d
            if first:
                l_s[rows, :] = part
                acc[rows, :] = pv
            else:
                al = jnp.exp2((m0 - m) * coef)
                l_s[rows, :] = l_s[rows, :] * al + part
                acc[rows, :] = acc[rows, :] * al + pv
            m_s[rows, :] = m

    step([c + nblk if rev else c], True, True)
    count = (2 * nblk - 1 - c) if rev else c
    idx = (lambda t: jnp.where(t < nblk, t, t + c + 1)) if rev else (lambda t: t)

    @pl.loop(0, count // PAIR)
    def _(t):
        step([idx(PAIR * t + u) for u in range(PAIR)], False, False)

    if PAIR > 1:
        @pl.loop(count // PAIR * PAIR, count)
        def _(t):
            step([idx(t)], False, False)
    for h in range(heads):
        rows = slice(h * piece, (h + 1) * piece)
        l = jnp.sum(l_s[rows, :], axis=1, keepdims=True)
        o_ref[:, h * DH:(h + 1) * DH] = (acc[rows, :] / l).astype(o_ref.dtype)


def attend(rev, npiece, nblk, c, q, *kvs):
    n, w = q.shape[0] // 2, q.shape[1]
    piece = n // npiece
    off = npiece if rev else 0
    heads = w // DH
    units = (nblk + 1 + nblk // 2) if rev else nblk // 2 + 1
    blocks = len(kvs) * nblk
    gs = pltpu.PrefetchScalarGridSpec(
        num_scalar_prefetch=1,
        grid=(npiece,),
        in_specs=[pl.BlockSpec((piece, w), lambda g, c: (g + off, 0))]
        + [pl.BlockSpec(memory_space=pl.ANY) for kv in kvs],
        out_specs=pl.BlockSpec((piece, w), lambda g, c: (g, 0)),
        scratch_shapes=[
            pltpu.VMEM((blocks * n, 2 * DH), jnp.bfloat16),
            pltpu.VMEM((blocks, DH, n), jnp.bfloat16),
            pltpu.VMEM((heads * piece, DH), jnp.bfloat16),
        ] + [pltpu.VMEM((heads * piece, DH), jnp.float32)] * 3 + [pltpu.SemaphoreType.DMA((2,))],
    )
    return pl.pallas_call(
        functools.partial(attn_body, rev, npiece, nblk),
        grid_spec=gs,
        out_shape=jax.ShapeDtypeStruct((n, w), jnp.bfloat16),
        compiler_params=pltpu.CompilerParams(dimension_semantics=("arbitrary",)),
        cost_estimate=pl.CostEstimate(
            flops=units * heads * n * n * DH * 4 * 3, bytes_accessed=3 * n * w * 2 + sum(kv.size * 2 for kv in kvs),
            transcendentals=units * heads * n * n),
        name="attn_b" if rev else "attn_a",
    )(c, q, *kvs)


def solution(mesh):
    tok = P(('dp', 'cp', 'tp'), None)
    col = P(None, 'tp')
    row = P('tp', None)
    ntp = mesh.shape['tp']
    ncp = mesh.shape['cp']

    def local(x, pos, g1, g2, wq, wk, wv, wo, w1, w3, w2):
        f32 = jnp.float32
        half = x.shape[0] // 2
        xs = [x[:half], x[half:]]
        bar = lax.optimization_barrier
        cidx = lax.axis_index('cp').astype(jnp.int32).reshape(1)
        ag = lambda u: lax.all_gather(u, 'tp', axis=0, tiled=True)
        rs = lambda u: lax.psum_scatter(u, 'tp', scatter_dimension=0, tiled=True)

        a = ag(rms_norm(x, g1)).reshape(ntp, 2, half, -1)
        pg = lax.all_gather(pos, 'tp', axis=0).reshape(ntp, 2, half)
        wkv = jnp.concatenate([wk, wv], axis=1)
        tabs = [rope_tables(pg[:, i].reshape(-1)) for i in range(2)]
        kvs = [proj(a, i, wkv, *tabs[i], 1, 2 * DH) for i in range(2)]
        kvg = [lax.all_gather(kv, 'cp', axis=0, tiled=True) for kv in kvs]
        qs = jnp.concatenate([proj(a, i, wq, *tabs[i], 2, 2 * DH) for i in range(2)], axis=0)

        oa = attend(False, ntp, ncp, cidx, qs, kvg[0])
        ya = mm(oa, wo, wo.shape[1] // 2)
        ya, qs = bar((ya, qs))
        yb = mm(attend(True, ntp, ncp, cidx, qs, *kvg), wo, wo.shape[1] // 2)
        h0 = (xs[0].astype(f32) + rs(ya).astype(f32)).astype(jnp.bfloat16)
        b0 = rms_norm(h0, g2)
        yb, b0 = bar((yb, b0))
        b0 = ag(b0)
        yb = rs(yb)
        m0, yb = bar((gate_up(b0, w1, w3, 2 * DH), yb))
        h1 = (xs[1].astype(f32) + yb.astype(f32)).astype(jnp.bfloat16)
        b1 = rms_norm(h1, g2)
        m0, b1 = bar((m0, b1))
        z0 = mm(m0, w2, 2 * DH)
        m1 = gate_up(ag(b1), w1, w3, 2 * DH)
        out0 = (h0.astype(f32) + rs(z0).astype(f32)).astype(jnp.bfloat16)
        out1 = down_scatter(ntp, m1, w2, h1, 2 * DH)
        return jnp.concatenate([out0, out1], axis=0)

    return jax.shard_map(local, mesh=mesh, in_specs=(tok, P(('dp', 'cp', 'tp')), P(None), P(None), col, col, col, row, col, col, row), out_specs=tok, check_vma=False)
```
